32 devices in a mesh: row: 8 (over y, x, core), col: 4 (over z).
Axes of the slice: x: 2, y: 2, z: 4, core: 2. Of those that a mesh axis runs over, the one named last changes fastest.
Arguments:
- query_proj: bfloat16 [192, 192, 128], P('row', 'col'), may hold values from -8 to 8
- key_proj: bfloat16 [192, 192, 128], P('row', 'col'), may hold values from -8 to 8
- value_proj: bfloat16 [192, 192, 128], P('row', 'col'), may hold values from -6 to 6
- pair_bias: bfloat16 [4, 192, 192], P(None, 'col', 'row'), may hold values from -9 to 9
- pair_mask: int32 [192, 192], P('row', 'col'), may hold values 0 or 1
- grad_out: bfloat16 [192, 192, 128], P('row', 'col'), may hold values from -18 to 18
Outputs:
- grad_query: bfloat16 [192, 192, 128], P('row', 'col')
- grad_key: bfloat16 [192, 192, 128], P('row', 'col')
- grad_value: bfloat16 [192, 192, 128], P('row', 'col')
- grad_bias: float32 [4, 192, 192], P(None, 'col', 'row')
The draws below stay inside these ranges and needn't reach their ends.
All inputs are finite; a program needn't handle non-finite values. No bound on the sum of `pair_mask` on one device may be relied on, other than what follows from the above.
Results may differ from the reference program's by a relative error of at most 0.0096.
Values may be sent and summed in bfloat16 or wider, within the bound.
A program may use at most 128 MiB of HBM per device.

```python
import math
import jax
import jax.numpy as jnp
from jax import lax

HEADS = 4
HEAD_DIM = 32
RESIDUES = 192
CHANNELS = 128


def field_draw(key):
    return jnp.clip(jax.random.normal(key, (RESIDUES, RESIDUES, CHANNELS), jnp.float32), -6.0, 6.0)


def draw_query_proj(key, part):
    values_drawn = field_draw(jax.random.fold_in(key, 1))
    return values_drawn.astype(jnp.bfloat16)


def draw_key_proj(key, part):
    values_drawn = field_draw(jax.random.fold_in(key, 2))
    return values_drawn.astype(jnp.bfloat16)


def place_ends(values, own_key, least, top_value):
    dims = values.shape
    index_at = [jax.random.randint(jax.random.fold_in(own_key, axis), (), 0, dims[axis]) for axis in range(len(dims))]
    values = values.at[tuple(index_at)].set(least)
    longest = dims.index(max(dims))
    index_at[longest] = (index_at[longest] + 1) % dims[longest]
    return values.at[tuple(index_at)].set(top_value)


def steps_of(own_key, extent, split, least, largest):
    loudness, own = 1.0, jax.random.fold_in(own_key, 6)
    for dim, shards_of in split:
        heights = jnp.exp(jax.random.uniform(jax.random.fold_in(own, dim), (shards_of,), jnp.float32, least / len(split), largest / len(split)))
        loudness = loudness * jnp.repeat(heights, extent[dim] // shards_of).reshape([-1 if axis == dim else 1 for axis in range(len(extent))])
    return loudness


def noise(key, shape, deviation, limit, cuts=(), held_as=jnp.bfloat16):
    level = steps_of(key, shape, cuts, -0.22, 0.18) if cuts else 1.0
    result = jax.random.normal(key, shape, jnp.float32) * deviation * level
    return jnp.minimum(jnp.maximum(result, -limit), limit).astype(held_as)


def setup_inputs(seed: int = 0) -> dict:
    seeds = jax.random.split(jax.random.key(seed), 7)
    query_proj = draw_query_proj(jax.random.fold_in(seeds[6], 71), 0)
    key_proj = draw_key_proj(jax.random.fold_in(seeds[6], 71), 0)
    value_proj = noise(seeds[2], (RESIDUES, RESIDUES, CHANNELS), 1.0, 6.0, ((0, 8), (1, 4)))
    pair_bias = noise(seeds[3], (HEADS, RESIDUES, RESIDUES), 1.5, 9.0, ((1, 4), (2, 8)))
    pair_mask = place_ends((jax.random.randint(seeds[4], (RESIDUES, RESIDUES), 0, 4) < 3).astype(jnp.int32), jax.random.fold_in(seeds[4], 1), 0, 1)
    grad_out = noise(seeds[5], (RESIDUES, RESIDUES, CHANNELS), 3.0, 18.0, ((0, 8), (1, 4)))
    return {"query_proj": query_proj, "key_proj": key_proj, "value_proj": value_proj, "pair_bias": pair_bias, "pair_mask": pair_mask, "grad_out": grad_out}


def block_grads(queries, keys_all, values_all, grads, mask_all, bias_full):
    block_rows, query_count, channel_count = queries.shape
    key_count = keys_all.shape[1]
    scale = 1.0 / math.sqrt(HEAD_DIM)
    query_heads = queries.astype(jnp.float32).reshape(block_rows, query_count, HEADS, HEAD_DIM)
    key_heads = keys_all.astype(jnp.float32).reshape(block_rows, key_count, HEADS, HEAD_DIM)
    value_heads = values_all.astype(jnp.float32).reshape(block_rows, key_count, HEADS, HEAD_DIM)
    grad_heads = grads.astype(jnp.float32).reshape(block_rows, query_count, HEADS, HEAD_DIM)
    masked = 1000000000.0 * (mask_all.astype(jnp.float32) - 1.0)
    scores = jnp.einsum('bjhd,bkhd->bhjk', query_heads, key_heads) * scale
    scores = scores + bias_full.astype(jnp.float32)[None] + masked[:, None, None, :]
    top_score = lax.optimization_barrier(jnp.max(scores, axis=-1, keepdims=True))
    weights = jnp.exp(scores - top_score)
    attn_probs = weights / lax.optimization_barrier(jnp.sum(weights, axis=-1, keepdims=True))
    attn_low = attn_probs.astype(jnp.bfloat16).astype(jnp.float32)
    attended = jnp.einsum('bhjk,bkhd->bjhd', attn_low, value_heads)
    row_delta = lax.optimization_barrier(jnp.sum(grad_heads * attended, axis=-1))
    grad_probs = jnp.einsum('bjhd,bkhd->bhjk', grad_heads, value_heads)
    grad_scores = attn_probs * (grad_probs - jnp.transpose(row_delta, (0, 2, 1))[..., None])
    scores_low = grad_scores.astype(jnp.bfloat16).astype(jnp.float32)
    grad_queries = jnp.einsum('bhjk,bkhd->bjhd', scores_low, key_heads) * scale
    grad_keys = jnp.einsum('bhjk,bjhd->bkhd', scores_low, query_heads) * scale
    grad_values = jnp.einsum('bhjk,bjhd->bkhd', attn_low, grad_heads)
    bias_grad = lax.optimization_barrier(jnp.sum(grad_scores, axis=0))
    return (grad_queries.reshape(block_rows, query_count, channel_count), grad_keys.reshape(block_rows, key_count, channel_count), grad_values.reshape(block_rows, key_count, channel_count), bias_grad)

def reference(query_proj, key_proj, value_proj, pair_bias, pair_mask, grad_out):
    block_rows = math.gcd(RESIDUES, 8)
    steps_count = RESIDUES // block_rows

    def split_rows(array):
        return array.reshape((steps_count, block_rows) + array.shape[1:])

    def one_block(bias_sum, pieces):
        grad_queries, grad_keys, grad_values, bias_grad = block_grads(pieces[0], pieces[1], pieces[2], pieces[3], pieces[4], pair_bias)
        return (bias_sum + bias_grad, (grad_queries.astype(jnp.bfloat16), grad_keys.astype(jnp.bfloat16), grad_values.astype(jnp.bfloat16)))
    start_sum = jnp.zeros((HEADS, RESIDUES, RESIDUES), jnp.float32)
    bias_sum, stacked = lax.scan(one_block, start_sum, (split_rows(query_proj), split_rows(key_proj), split_rows(value_proj), split_rows(grad_out), split_rows(pair_mask)))
    full_shape = (RESIDUES, RESIDUES, CHANNELS)
    return (stacked[0].reshape(full_shape), stacked[1].reshape(full_shape), stacked[2].reshape(full_shape), bias_sum)
```

```python
import functools
import math

import jax
import jax.numpy as jnp
from jax import lax
from jax.experimental import pallas as pl
from jax.experimental.pallas import tpu as pltpu
from jax.sharding import PartitionSpec as P

HEADS = 4
HEAD_DIM = 32


def block_grads(queries, keys_all, values_all, grads, mask_all, bias_full):
    block_rows, query_count, channel_count = queries.shape
    key_count = keys_all.shape[1]
    scale = 1.0 / math.sqrt(HEAD_DIM)
    query_heads = queries.reshape(block_rows, query_count, HEADS, HEAD_DIM)
    key_heads = keys_all.reshape(block_rows, key_count, HEADS, HEAD_DIM)
    value_heads = values_all.reshape(block_rows, key_count, HEADS, HEAD_DIM)
    grad_heads = grads.reshape(block_rows, query_count, HEADS, HEAD_DIM)
    masked = 1000000000.0 * (mask_all.astype(jnp.float32) - 1.0)
    scores = (
        jnp.einsum("bjhd,bkhd->bhjk", query_heads, key_heads, preferred_element_type=jnp.float32)
        * scale
    )
    scores = scores + bias_full.astype(jnp.float32)[None] + masked[:, None, None, :]
    top_score = jnp.max(scores, axis=-1, keepdims=True)
    weights = jnp.exp(scores - top_score)
    attn_probs = weights / jnp.sum(weights, axis=-1, keepdims=True)
    attn_low = attn_probs.astype(jnp.bfloat16)
    attended = jnp.einsum(
        "bhjk,bkhd->bjhd", attn_low, value_heads, preferred_element_type=jnp.float32
    )
    row_delta = jnp.sum(grad_heads.astype(jnp.float32) * attended, axis=-1)
    grad_probs = jnp.einsum(
        "bjhd,bkhd->bhjk", grad_heads, value_heads, preferred_element_type=jnp.float32
    )
    grad_scores = attn_probs * (grad_probs - jnp.transpose(row_delta, (0, 2, 1))[..., None])
    scores_low = grad_scores.astype(jnp.bfloat16)
    grad_queries = (
        jnp.einsum("bhjk,bkhd->bjhd", scores_low, key_heads, preferred_element_type=jnp.float32)
        * scale
    )
    grad_keys = (
        jnp.einsum("bhjk,bjhd->bkhd", scores_low, query_heads, preferred_element_type=jnp.float32)
        * scale
    )
    grad_values = jnp.einsum(
        "bhjk,bjhd->bkhd", attn_low, grad_heads, preferred_element_type=jnp.float32
    )
    bias_grad = jnp.sum(grad_scores, axis=0)
    return (
        grad_queries.reshape(block_rows, query_count, channel_count),
        grad_keys.reshape(block_rows, key_count, channel_count),
        grad_values.reshape(block_rows, key_count, channel_count),
        bias_grad,
    )


def all_blocks(queries, keys_all, values_all, grads, mask_all, bias_full):
    row_count, query_count, channel_count = queries.shape
    key_count = keys_all.shape[1]
    block_rows = 1
    while (
        block_rows * 2 <= row_count
        and row_count % (block_rows * 2) == 0
        and (block_rows * query_count < 512)
    ):
        block_rows = block_rows * 2
    steps_count = row_count // block_rows

    def split_rows(array):
        return array.reshape((steps_count, block_rows) + array.shape[1:])

    def one_block(bias_sum, pieces):
        grad_queries, grad_keys, grad_values, bias_grad = block_grads(
            pieces[0], pieces[1], pieces[2], pieces[3], pieces[4], bias_full
        )
        return (bias_sum + bias_grad, (grad_queries, grad_keys, grad_values))

    start_sum = jnp.zeros((HEADS, query_count, key_count), jnp.float32)
    bias_sum, stacked = lax.scan(
        one_block,
        start_sum,
        (
            split_rows(queries),
            split_rows(keys_all),
            split_rows(values_all),
            split_rows(grads),
            split_rows(mask_all),
        ),
    )
    return (
        stacked[0].reshape(row_count, query_count, channel_count),
        stacked[1].reshape(row_count, key_count, channel_count),
        stacked[2].reshape(row_count, key_count, channel_count),
        bias_sum,
    )


def local(query_proj, key_proj, value_proj, pair_bias, pair_mask, grad_out):
    bias_rows = lax.all_gather(pair_bias, "row", axis=2, tiled=True)
    mask_low = pair_mask.astype(jnp.bfloat16)
    local_tiles = (
        lax.all_to_all(query_proj, "col", split_axis=0, concat_axis=1, tiled=True),
        lax.all_to_all(key_proj, "col", split_axis=0, concat_axis=1, tiled=True),
        lax.all_to_all(value_proj, "col", split_axis=0, concat_axis=1, tiled=True),
        lax.all_to_all(grad_out, "col", split_axis=0, concat_axis=1, tiled=True),
        lax.all_to_all(mask_low, "col", split_axis=0, concat_axis=1, tiled=True),
    )
    bias_full = lax.all_gather(bias_rows, "col", axis=1, tiled=True)
    grad_queries, grad_keys, grad_values, bias_whole = all_blocks(
        local_tiles[0], local_tiles[1], local_tiles[2], local_tiles[3], local_tiles[4], bias_full
    )
    grad_query, grad_key, grad_value = (
        lax.all_to_all(
            grad_queries.astype(jnp.bfloat16), "col", split_axis=1, concat_axis=0, tiled=True
        ),
        lax.all_to_all(
            grad_keys.astype(jnp.bfloat16), "col", split_axis=1, concat_axis=0, tiled=True
        ),
        lax.all_to_all(
            grad_values.astype(jnp.bfloat16), "col", split_axis=1, concat_axis=0, tiled=True
        ),
    )
    bias_part = lax.psum_scatter(bias_whole, "col", scatter_dimension=1, tiled=True)
    grad_bias = lax.psum_scatter(bias_part, "row", scatter_dimension=2, tiled=True)
    return (grad_query, grad_key, grad_value, grad_bias)


MESH = pl.DeviceIdType.MESH


def round_up(value, step):
    return -(-value // step) * step


def fused_kernel(
    rows_n, cols_n, pack,
    q_ref, k_ref, v_ref, g_ref, bias_ref, mask_ref,
    gq_ref, gk_ref, gv_ref, gb_ref,
    got, stage, bias_all, mask_all, bias_full, bias_sum, part, part_in, tile, tile_in,
    in_send, in_recv, out_send, out_recv, bc_send, bc_recv, br_send, br_recv,
    mk_send, mk_recv, pr_send, pr_recv, pc_send, pc_recv, own_sem,
):
    row, col = lax.axis_index("row"), lax.axis_index("col")
    per = got.shape[1]
    count = got.shape[2]
    width = q_ref.shape[1]
    keys = bias_sum.shape[1] // rows_n
    packs, padded, lanes = bias_ref.shape
    chunk = 2 if per % 2 == 0 else 1
    chunks = per // chunk
    scale = 1.0 / math.sqrt(HEAD_DIM)
    sources = (q_ref, k_ref, v_ref, g_ref)
    results = (gq_ref, gk_ref, gv_ref)

    def row_peer(d):
        return (lax.rem(row + d, rows_n), col)

    def col_peer(d):
        return (row, lax.rem(col + d, cols_n))

    def remote(src, dst, send, recv, peer):
        return pltpu.make_async_remote_copy(
            src_ref=src, dst_ref=dst, send_sem=send, recv_sem=recv,
            device_id=peer, device_id_type=MESH,
        )

    barrier = pltpu.get_barrier_semaphore()
    for d in range(1, rows_n):
        pl.semaphore_signal(barrier, inc=1, device_id=row_peer(d), device_id_type=MESH)
    for d in range(1, cols_n):
        pl.semaphore_signal(barrier, inc=1, device_id=col_peer(d), device_id_type=MESH)
    pl.semaphore_wait(barrier, rows_n + cols_n - 2)

    my_cols = pl.ds(pl.multiple_of(col * width, width), width)
    bias_col = [
        remote(bias_ref, bias_all.at[row, col], bc_send.at[d], bc_recv.at[d], col_peer(d))
        for d in range(1, cols_n)
    ]
    mask_col = [
        remote(mask_ref, mask_all.at[my_cols], mk_send.at[d], mk_recv.at[d], col_peer(d))
        for d in range(1, cols_n)
    ]
    for copy in bias_col + mask_col:
        copy.start()
    own = [
        pltpu.make_async_copy(bias_ref, bias_all.at[row, col], own_sem.at[0]),
        pltpu.make_async_copy(mask_ref, mask_all.at[my_cols], own_sem.at[1]),
    ]
    for a in range(4):
        own.append(pltpu.make_async_copy(
            sources[a].at[pl.ds(col * per, per)], got.at[a, :, my_cols], own_sem.at[2 + a]
        ))
    for copy in own:
        copy.start()

    def in_copies(c):
        copies = []
        for d in range(1, cols_n):
            peer = col_peer(d)
            for a in range(4):
                copies.append(remote(
                    sources[a].at[pl.ds(peer[1] * per + c * chunk, chunk)],
                    got.at[a, pl.ds(c * chunk, chunk), my_cols],
                    in_send.at[c, d, a], in_recv.at[c, d, a], peer,
                ))
        return copies

    def out_copies(c):
        copies = []
        for d in range(1, cols_n):
            peer = col_peer(d)
            there = pl.ds(pl.multiple_of(peer[1] * width, width), width)
            for a in range(3):
                copies.append(remote(
                    stage.at[a, pl.ds(c * chunk, chunk), there],
                    results[a].at[pl.ds(col * per + c * chunk, chunk)],
                    out_send.at[c, d, a], out_recv.at[c, d, a], peer,
                ))
        return copies

    def own_outs(c):
        return [
            pltpu.make_async_copy(
                stage.at[a, pl.ds(c * chunk, chunk), my_cols],
                results[a].at[pl.ds(col * per + c * chunk, chunk)],
                out_send.at[c, 0, a],
            )
            for a in range(3)
        ]

    @pl.loop(0, chunks)
    def _(c):
        for copy in in_copies(c):
            copy.start()

    for copy in bias_col:
        copy.wait_recv()
    for copy in own:
        copy.wait()
    bias_row = [
        remote(bias_all.at[row], bias_all.at[row], br_send.at[d], br_recv.at[d], row_peer(d))
        for d in range(1, rows_n)
    ]
    for copy in bias_row:
        copy.start()
    bias_sum[...] = jnp.zeros_like(bias_sum)
    part[...] = jnp.zeros_like(part)
    for copy in mask_col:
        copy.wait_recv()
    for copy in bias_row:
        copy.wait_recv()

    def pick(z, hh, shape, lane_axis):
        lane = lax.broadcasted_iota(jnp.int32, shape, lane_axis)
        at = lax.broadcasted_iota(jnp.int32, shape, 1 - lane_axis)
        inside = (lane >= hh * width) & (lane < (hh + 1) * width)
        return jnp.where(inside & (lane + (z - hh) * width == at), 1.0, 0.0).astype(jnp.bfloat16)

    for p in range(packs):
        for hh in range(pack):
            whole = jnp.zeros((rows_n * padded, count), jnp.float32)
            for z in range(cols_n):
                piece = bias_all[:, z, p].reshape(rows_n * padded, lanes)
                whole = whole + jnp.dot(
                    piece, pick(z, hh, (lanes, count), 0), preferred_element_type=jnp.float32
                )
            for r in range(rows_n):
                bias_full[p * pack + hh, r * keys:(r + 1) * keys, :] = (
                    whole[r * padded:r * padded + keys]
                )

    nt = (((1,), (1,)), ((), ()))
    tn = (((0,), (0,)), ((), ()))
    channel = lax.broadcasted_iota(jnp.int32, (count, HEADS * HEAD_DIM), 1)
    mask_lane = lax.broadcasted_iota(jnp.int32, mask_all.shape, 1)

    def one_row(i):
        q, k, v, g = got[0, i], got[1, i], got[2, i], got[3, i]
        present = jnp.sum(
            jnp.where(mask_lane == col * per + i, mask_all[...].astype(jnp.float32), 0.0),
            axis=1, keepdims=True,
        )
        masked = 1000000000.0 * (present - 1.0)
        gq = jnp.zeros((count, HEADS * HEAD_DIM), jnp.float32)
        gk = gq
        gv = gq
        for h in range(HEADS):
            mine = (channel >= h * HEAD_DIM) & (channel < (h + 1) * HEAD_DIM)

            def only(x):
                return jnp.where(mine, x, jnp.zeros_like(x))

            kh, vh, qh, gh = only(k), only(v), only(q), only(g)
            scores = lax.dot_general(kh, q, nt, preferred_element_type=jnp.float32) * scale
            scores = scores + bias_full[h] + masked
            weights = jnp.exp(scores - jnp.max(scores, axis=0, keepdims=True))
            probs = weights * (1.0 / jnp.sum(weights, axis=0, keepdims=True))
            low = probs.astype(jnp.bfloat16)
            grad_probs = lax.dot_general(vh, g, nt, preferred_element_type=jnp.float32)
            delta = jnp.sum(low.astype(jnp.float32) * grad_probs, axis=0, keepdims=True)
            grad_scores = probs * (grad_probs - delta)
            bias_sum[h] += grad_scores
            slow = grad_scores.astype(jnp.bfloat16)
            gq = gq + lax.dot_general(slow, kh, tn, preferred_element_type=jnp.float32)
            gk = gk + jnp.dot(slow, qh, preferred_element_type=jnp.float32)
            gv = gv + jnp.dot(low, gh, preferred_element_type=jnp.float32)
        stage[0, i] = (gq * scale).astype(jnp.bfloat16)
        stage[1, i] = (gk * scale).astype(jnp.bfloat16)
        stage[2, i] = gv.astype(jnp.bfloat16)

    @pl.loop(0, chunks)
    def _(c):
        for copy in in_copies(c):
            copy.wait_recv()

        @pl.loop(0, chunk)
        def _(r):
            one_row(c * chunk + r)

        for copy in out_copies(c) + own_outs(c):
            copy.start()

    for r in range(rows_n):
        for h in range(HEADS):
            part[r, h, 0:keys, :] = bias_sum[h, r * keys:(r + 1) * keys, :].astype(jnp.bfloat16)
    part_row = []
    for d in range(1, rows_n):
        peer = row_peer(d)
        part_row.append(remote(
            part.at[peer[0]], part_in.at[row], pr_send.at[d], pr_recv.at[d], peer
        ))
    for copy in part_row:
        copy.start()
    for copy in part_row:
        copy.wait_recv()
    sums = []
    for h in range(HEADS):
        total = part[row, h].astype(jnp.float32)
        for d in range(1, rows_n):
            total = total + part_in[lax.rem(row + d, rows_n), h].astype(jnp.float32)
        sums.append(total.astype(jnp.bfloat16))
    for z in range(cols_n):
        for p in range(packs):
            packed = jnp.zeros((padded, lanes), jnp.float32)
            for hh in range(pack):
                packed = packed + jnp.dot(
                    sums[p * pack + hh], pick(z, hh, (count, lanes), 1),
                    preferred_element_type=jnp.float32,
                )
            tile[z, p] = packed.astype(jnp.bfloat16)
    part_col = []
    for d in range(1, cols_n):
        peer = col_peer(d)
        part_col.append(remote(
            tile.at[peer[1]], tile_in.at[col], pc_send.at[d], pc_recv.at[d], peer
        ))
    for copy in part_col:
        copy.start()
    for copy in part_col:
        copy.wait_recv()
    total = tile[col].astype(jnp.float32)
    for d in range(1, cols_n):
        total = total + tile_in[lax.rem(col + d, cols_n)].astype(jnp.float32)
    gb_ref[...] = total

    @pl.loop(0, chunks)
    def _(c):
        for copy in in_copies(c):
            copy.wait_send()
        for copy in out_copies(c):
            copy.wait()
        for copy in own_outs(c):
            copy.wait()

    for copy in bias_col + mask_col + bias_row + part_row + part_col:
        copy.wait_send()


def fused(rows_n, cols_n, query_proj, key_proj, value_proj, pair_bias, pair_mask, grad_out):
    rows, width, channels = query_proj.shape
    keys = pair_bias.shape[2]
    per, count = rows // cols_n, width * cols_n
    pack = 1
    while pack * 2 <= HEADS and pack * 2 * width <= 128:
        pack = pack * 2
    packs = HEADS // pack
    padded, lanes = round_up(keys, 16), round_up(pack * width, 128)
    flipped = jnp.transpose(pair_bias, (0, 2, 1)).reshape(packs, pack, keys, width)
    flipped = jnp.transpose(flipped, (0, 2, 1, 3)).reshape(packs, keys, pack * width)
    flipped = jnp.pad(flipped, ((0, 0), (0, padded - keys), (0, lanes - pack * width)))
    mask_low = jnp.transpose(pair_mask).astype(jnp.bfloat16)
    mask_low = jnp.pad(mask_low, ((0, 0), (0, round_up(rows, 128) - rows)))
    chunk = 2 if per % 2 == 0 else 1
    chunks = per // chunk
    bf16, f32 = jnp.bfloat16, jnp.float32
    anywhere = pl.BlockSpec(memory_space=pl.ANY)
    on_chip = pl.BlockSpec(memory_space=pltpu.VMEM)
    sem = pltpu.SemaphoreType.DMA
    tile_shape = jax.ShapeDtypeStruct(query_proj.shape, bf16)
    gq, gk, gv, gb = pl.pallas_call(
        functools.partial(fused_kernel, rows_n, cols_n, pack),
        name="triangle_grads",
        out_shape=(
            tile_shape, tile_shape, tile_shape,
            jax.ShapeDtypeStruct((packs, padded, lanes), f32),
        ),
        in_specs=[anywhere] * 4 + [on_chip] * 2,
        out_specs=(anywhere, anywhere, anywhere, on_chip),
        scratch_shapes=[
            pltpu.VMEM((4, per, count, channels), bf16),
            pltpu.VMEM((3, per, count, channels), bf16),
            pltpu.VMEM((rows_n, cols_n, packs, padded, lanes), bf16),
            pltpu.VMEM((count, mask_low.shape[1]), bf16),
            pltpu.VMEM((HEADS, count, count), f32),
            pltpu.VMEM((HEADS, count, count), f32),
            pltpu.VMEM((rows_n, HEADS, padded, count), bf16),
            pltpu.VMEM((rows_n, HEADS, padded, count), bf16),
            pltpu.VMEM((cols_n, packs, padded, lanes), bf16),
            pltpu.VMEM((cols_n, packs, padded, lanes), bf16),
            sem((chunks, cols_n, 4)), sem((chunks, cols_n, 4)),
            sem((chunks, cols_n, 3)), sem((chunks, cols_n, 3)),
            sem((cols_n,)), sem((cols_n,)),
            sem((rows_n,)), sem((rows_n,)),
            sem((cols_n,)), sem((cols_n,)),
            sem((rows_n,)), sem((rows_n,)),
            sem((cols_n,)), sem((cols_n,)),
            sem((6,)),
        ],
        compiler_params=pltpu.CompilerParams(collective_id=0, has_side_effects=True),
    )(query_proj, key_proj, value_proj, grad_out, flipped, mask_low)
    gb = gb[:, :keys, :pack * width].reshape(packs, keys, pack, width)
    gb = jnp.transpose(gb, (0, 2, 3, 1)).reshape(HEADS, width, keys)
    return gq, gk, gv, gb


def choose(rows_n, cols_n):
    def run(*arrays):
        count = arrays[0].shape[1] * cols_n
        if count * count * 4 <= 512 * 1024 and arrays[0].shape[0] % cols_n == 0:
            return fused(rows_n, cols_n, *arrays)
        return local(*arrays)

    return run


def solution(mesh):
    placed = (
        P("row", "col", None),
        P("row", "col", None),
        P("row", "col", None),
        P(None, "col", "row"),
        P("row", "col"),
        P("row", "col", None),
    )
    return jax.shard_map(
        choose(mesh.shape["row"], mesh.shape["col"]),
        mesh=mesh,
        in_specs=placed,
        out_specs=(
            P("row", "col", None),
            P("row", "col", None),
            P("row", "col", None),
            P(None, "col", "row"),
        ),
        check_vma=False,
    )
```

```python
import functools
import math

import jax
import jax.numpy as jnp
from jax import lax
from jax.experimental import pallas as pl
from jax.experimental.pallas import tpu as pltpu
from jax.sharding import PartitionSpec as P

HEADS = 4
HEAD_DIM = 32


def block_grads(queries, keys_all, values_all, grads, mask_all, bias_full):
    block_rows, query_count, channel_count = queries.shape
    key_count = keys_all.shape[1]
    scale = 1.0 / math.sqrt(HEAD_DIM)
    query_heads = queries.reshape(block_rows, query_count, HEADS, HEAD_DIM)
    key_heads = keys_all.reshape(block_rows, key_count, HEADS, HEAD_DIM)
    value_heads = values_all.reshape(block_rows, key_count, HEADS, HEAD_DIM)
    grad_heads = grads.reshape(block_rows, query_count, HEADS, HEAD_DIM)
    masked = 1000000000.0 * (mask_all.astype(jnp.float32) - 1.0)
    scores = (
        jnp.einsum("bjhd,bkhd->bhjk", query_heads, key_heads, preferred_element_type=jnp.float32)
        * scale
    )
    scores = scores + bias_full.astype(jnp.float32)[None] + masked[:, None, None, :]
    top_score = jnp.max(scores, axis=-1, keepdims=True)
    weights = jnp.exp(scores - top_score)
    attn_probs = weights / jnp.sum(weights, axis=-1, keepdims=True)
    attn_low = attn_probs.astype(jnp.bfloat16)
    attended = jnp.einsum(
        "bhjk,bkhd->bjhd", attn_low, value_heads, preferred_element_type=jnp.float32
    )
    row_delta = jnp.sum(grad_heads.astype(jnp.float32) * attended, axis=-1)
    grad_probs = jnp.einsum(
        "bjhd,bkhd->bhjk", grad_heads, value_heads, preferred_element_type=jnp.float32
    )
    grad_scores = attn_probs * (grad_probs - jnp.transpose(row_delta, (0, 2, 1))[..., None])
    scores_low = grad_scores.astype(jnp.bfloat16)
    grad_queries = (
        jnp.einsum("bhjk,bkhd->bjhd", scores_low, key_heads, preferred_element_type=jnp.float32)
        * scale
    )
    grad_keys = (
        jnp.einsum("bhjk,bjhd->bkhd", scores_low, query_heads, preferred_element_type=jnp.float32)
        * scale
    )
    grad_values = jnp.einsum(
        "bhjk,bjhd->bkhd", attn_low, grad_heads, preferred_element_type=jnp.float32
    )
    bias_grad = jnp.sum(grad_scores, axis=0)
    return (
        grad_queries.reshape(block_rows, query_count, channel_count),
        grad_keys.reshape(block_rows, key_count, channel_count),
        grad_values.reshape(block_rows, key_count, channel_count),
        bias_grad,
    )


def all_blocks(queries, keys_all, values_all, grads, mask_all, bias_full):
    row_count, query_count, channel_count = queries.shape
    key_count = keys_all.shape[1]
    block_rows = 1
    while (
        block_rows * 2 <= row_count
        and row_count % (block_rows * 2) == 0
        and (block_rows * query_count < 512)
    ):
        block_rows = block_rows * 2
    steps_count = row_count // block_rows

    def split_rows(array):
        return array.reshape((steps_count, block_rows) + array.shape[1:])

    def one_block(bias_sum, pieces):
        grad_queries, grad_keys, grad_values, bias_grad = block_grads(
            pieces[0], pieces[1], pieces[2], pieces[3], pieces[4], bias_full
        )
        return (bias_sum + bias_grad, (grad_queries, grad_keys, grad_values))

    start_sum = jnp.zeros((HEADS, query_count, key_count), jnp.float32)
    bias_sum, stacked = lax.scan(
        one_block,
        start_sum,
        (
            split_rows(queries),
            split_rows(keys_all),
            split_rows(values_all),
            split_rows(grads),
            split_rows(mask_all),
        ),
    )
    return (
        stacked[0].reshape(row_count, query_count, channel_count),
        stacked[1].reshape(row_count, key_count, channel_count),
        stacked[2].reshape(row_count, key_count, channel_count),
        bias_sum,
    )


def local(query_proj, key_proj, value_proj, pair_bias, pair_mask, grad_out):
    bias_rows = lax.all_gather(pair_bias, "row", axis=2, tiled=True)
    mask_low = pair_mask.astype(jnp.bfloat16)
    local_tiles = (
        lax.all_to_all(query_proj, "col", split_axis=0, concat_axis=1, tiled=True),
        lax.all_to_all(key_proj, "col", split_axis=0, concat_axis=1, tiled=True),
        lax.all_to_all(value_proj, "col", split_axis=0, concat_axis=1, tiled=True),
        lax.all_to_all(grad_out, "col", split_axis=0, concat_axis=1, tiled=True),
        lax.all_to_all(mask_low, "col", split_axis=0, concat_axis=1, tiled=True),
    )
    bias_full = lax.all_gather(bias_rows, "col", axis=1, tiled=True)
    grad_queries, grad_keys, grad_values, bias_whole = all_blocks(
        local_tiles[0], local_tiles[1], local_tiles[2], local_tiles[3], local_tiles[4], bias_full
    )
    grad_query, grad_key, grad_value = (
        lax.all_to_all(
            grad_queries.astype(jnp.bfloat16), "col", split_axis=1, concat_axis=0, tiled=True
        ),
        lax.all_to_all(
            grad_keys.astype(jnp.bfloat16), "col", split_axis=1, concat_axis=0, tiled=True
        ),
        lax.all_to_all(
            grad_values.astype(jnp.bfloat16), "col", split_axis=1, concat_axis=0, tiled=True
        ),
    )
    bias_part = lax.psum_scatter(bias_whole, "col", scatter_dimension=1, tiled=True)
    grad_bias = lax.psum_scatter(bias_part, "row", scatter_dimension=2, tiled=True)
    return (grad_query, grad_key, grad_value, grad_bias)


HELD_CHUNKS = 0
MESH = pl.DeviceIdType.MESH


def round_up(value, step):
    return -(-value // step) * step


def fused_kernel(
    rows_n, cols_n, pack,
    q_ref, k_ref, v_ref, g_ref, bias_in, mask_in,
    gq_ref, gk_ref, gv_ref, gb_ref,
    bias_ref, mask_ref, got, stage, bias_all, mask_all, bias_full, bias_sum, part, part_in, tile, tile_in,
    in_send, in_recv, out_send, out_recv, bc_send, bc_recv, br_send, br_recv,
    mk_send, mk_recv, pr_send, pr_recv, pc_send, pc_recv, own_sem,
):
    row, col = lax.axis_index("row"), lax.axis_index("col")
    per = got.shape[1]
    count = got.shape[2]
    width = q_ref.shape[1]
    keys = bias_sum.shape[1] // rows_n
    rows_here = mask_in.shape[0]
    packs, padded, lanes = bias_ref.shape
    chunk = 2 if per % 2 == 0 else 1
    chunks = per // chunk
    held = min(chunks, HELD_CHUNKS)
    scale = 1.0 / math.sqrt(HEAD_DIM)
    sources = (q_ref, k_ref, v_ref, g_ref)
    results = (gq_ref, gk_ref, gv_ref)

    def row_peer(d):
        return (lax.rem(row + d, rows_n), col)

    paired = cols_n & (cols_n - 1) == 0

    def col_peer(d):
        if not paired:
            return (row, lax.rem(col + d, cols_n))
        other = 0
        bit = 1
        while bit < cols_n:
            mine = lax.rem(col // bit, 2)
            other = other + bit * (1 - mine if d & bit else mine)
            bit = bit * 2
        return (row, other)

    def remote(src, dst, send, recv, peer):
        return pltpu.make_async_remote_copy(
            src_ref=src, dst_ref=dst, send_sem=send, recv_sem=recv,
            device_id=peer, device_id_type=MESH,
        )

    nn = (((1,), (0,)), ((), ()))
    nt = (((1,), (1,)), ((), ()))
    tn = (((0,), (0,)), ((), ()))
    barrier = pltpu.get_barrier_semaphore()
    for d in range(1, rows_n):
        pl.semaphore_signal(barrier, inc=1, device_id=row_peer(d), device_id_type=MESH)
    for d in range(1, cols_n):
        pl.semaphore_signal(barrier, inc=1, device_id=col_peer(d), device_id_type=MESH)

    def shifted(shape, shift):
        at = lax.broadcasted_iota(jnp.int32, shape, 0)
        lane = lax.broadcasted_iota(jnp.int32, shape, 1)
        return jnp.where(lane == at + shift, 1.0, 0.0).astype(jnp.bfloat16)

    bias_ref[...] = jnp.zeros_like(bias_ref)
    for p in range(packs):
        flipped = jnp.zeros((keys, lanes), jnp.float32)
        for hh in range(pack):
            flipped = flipped + lax.dot_general(
                bias_in[p * pack + hh], shifted((width, lanes), hh * width), nn,
                preferred_element_type=jnp.float32,
            )
        bias_ref[p, 0:keys, :] = flipped.astype(jnp.bfloat16)
    mask_ref[...] = lax.dot_general(
        mask_in[...].astype(jnp.float32).astype(jnp.bfloat16),
        shifted((rows_here, mask_ref.shape[1]), 0), tn,
        preferred_element_type=jnp.float32,
    ).astype(jnp.bfloat16)
    pl.semaphore_wait(barrier, rows_n + cols_n - 2)

    my_cols = pl.ds(pl.multiple_of(col * width, width), width)
    bias_col = [
        remote(bias_ref, bias_all.at[row, col], bc_send.at[d], bc_recv.at[d], col_peer(d))
        for d in range(1, cols_n)
    ]
    mask_col = [
        remote(mask_ref, mask_all.at[my_cols], mk_send.at[d], mk_recv.at[d], col_peer(d))
        for d in range(1, cols_n)
    ]
    for copy in bias_col + mask_col:
        copy.start()
    own = [
        pltpu.make_async_copy(bias_ref, bias_all.at[row, col], own_sem.at[0]),
        pltpu.make_async_copy(mask_ref, mask_all.at[my_cols], own_sem.at[1]),
    ]
    for a in range(4):
        own.append(pltpu.make_async_copy(
            sources[a].at[pl.ds(col * per, per)], got.at[a, :, my_cols], own_sem.at[2 + a]
        ))
    for copy in own:
        copy.start()

    def in_copies(c):
        copies = []
        for d in reversed(range(1, cols_n)):
            peer = col_peer(d)
            for a in range(4):
                copies.append(remote(
                    sources[a].at[pl.ds(peer[1] * per + c * chunk, chunk)],
                    got.at[a, pl.ds(c * chunk, chunk), my_cols],
                    in_send.at[c, d, a], in_recv.at[c, d, a], peer,
                ))
        return copies

    def out_copies(c):
        copies = []
        for d in reversed(range(1, cols_n)):
            peer = col_peer(d)
            there = pl.ds(pl.multiple_of(peer[1] * width, width), width)
            for a in range(3):
                copies.append(remote(
                    stage.at[a, pl.ds(c * chunk, chunk), there],
                    results[a].at[pl.ds(col * per + c * chunk, chunk)],
                    out_send.at[c, d, a], out_recv.at[c, d, a], peer,
                ))
        return copies

    def own_outs(c):
        return [
            pltpu.make_async_copy(
                stage.at[a, pl.ds(c * chunk, chunk), my_cols],
                results[a].at[pl.ds(col * per + c * chunk, chunk)],
                out_send.at[c, 0, a],
            )
            for a in range(3)
        ]

    @pl.loop(0, chunks)
    def _(c):
        for copy in in_copies(c):
            copy.start()

    for copy in bias_col:
        copy.wait_recv()
    for copy in own:
        copy.wait()
    bias_row = [
        remote(bias_all.at[row], bias_all.at[row], br_send.at[d], br_recv.at[d], row_peer(d))
        for d in range(1, rows_n)
    ]
    for copy in bias_row:
        copy.start()
    bias_sum[...] = jnp.zeros_like(bias_sum)
    part[...] = jnp.zeros_like(part)
    for copy in mask_col:
        copy.wait_recv()
    for copy in bias_row:
        copy.wait_recv()

    def pick(z, hh, shape, lane_axis):
        lane = lax.broadcasted_iota(jnp.int32, shape, lane_axis)
        at = lax.broadcasted_iota(jnp.int32, shape, 1 - lane_axis)
        inside = (lane >= hh * width) & (lane < (hh + 1) * width)
        return jnp.where(inside & (lane + (z - hh) * width == at), 1.0, 0.0).astype(jnp.bfloat16)

    for p in range(packs):
        for hh in range(pack):
            whole = jnp.zeros((rows_n * padded, count), jnp.float32)
            for z in range(cols_n):
                piece = bias_all[:, z, p].reshape(rows_n * padded, lanes)
                whole = whole + jnp.dot(
                    piece, pick(z, hh, (lanes, count), 0), preferred_element_type=jnp.float32
                )
            for r in range(rows_n):
                bias_full[p * pack + hh, r * keys:(r + 1) * keys, :] = (
                    whole[r * padded:r * padded + keys]
                )

    channel = lax.broadcasted_iota(jnp.int32, (count, HEADS * HEAD_DIM), 1)
    mask_lane = lax.broadcasted_iota(jnp.int32, mask_all.shape, 1)

    def one_row(i):
        q, k, v, g = got[0, i], got[1, i], got[2, i], got[3, i]
        present = jnp.sum(
            jnp.where(mask_lane == col * per + i, mask_all[...].astype(jnp.float32), 0.0),
            axis=1, keepdims=True,
        )
        masked = 1000000000.0 * (present - 1.0)
        gq = jnp.zeros((count, HEADS * HEAD_DIM), jnp.float32)
        gk = gq
        gv = gq
        for h in range(HEADS):
            mine = (channel >= h * HEAD_DIM) & (channel < (h + 1) * HEAD_DIM)

            def only(x):
                return jnp.where(mine, x, jnp.zeros_like(x))

            kh, vh, qh, gh = only(k), only(v), only(q), only(g)
            scores = lax.dot_general(kh, q, nt, preferred_element_type=jnp.float32) * scale
            scores = scores + bias_full[h] + masked
            weights = jnp.exp(scores - jnp.max(scores, axis=0, keepdims=True))
            probs = weights * (1.0 / jnp.sum(weights, axis=0, keepdims=True))
            low = probs.astype(jnp.bfloat16)
            grad_probs = lax.dot_general(vh, g, nt, preferred_element_type=jnp.float32)
            delta = jnp.sum(low.astype(jnp.float32) * grad_probs, axis=0, keepdims=True)
            grad_scores = probs * (grad_probs - delta)
            bias_sum[h] += grad_scores
            slow = grad_scores.astype(jnp.bfloat16)
            gq = gq + lax.dot_general(slow, kh, tn, preferred_element_type=jnp.float32)
            gk = gk + jnp.dot(slow, qh, preferred_element_type=jnp.float32)
            gv = gv + jnp.dot(low, gh, preferred_element_type=jnp.float32)
        stage[0, i] = (gq * scale).astype(jnp.bfloat16)
        stage[1, i] = (gk * scale).astype(jnp.bfloat16)
        stage[2, i] = gv.astype(jnp.bfloat16)

    @pl.loop(0, chunks)
    def _(c):
        for copy in in_copies(c):
            copy.wait_recv()

        @pl.loop(0, chunk)
        def _(r):
            one_row(c * chunk + r)

        for copy in own_outs(c):
            copy.start()

        @pl.when(c < chunks - held)
        def _():
            for copy in out_copies(c):
                copy.start()

    for r in range(rows_n):
        for h in range(HEADS):
            part[r, h, 0:keys, :] = bias_sum[h, r * keys:(r + 1) * keys, :].astype(jnp.bfloat16)
    part_row = []
    for d in range(1, rows_n):
        peer = row_peer(d)
        part_row.append(remote(
            part.at[peer[0]], part_in.at[row], pr_send.at[d], pr_recv.at[d], peer
        ))
    for copy in part_row:
        copy.start()
    for copy in part_row:
        copy.wait_recv()
    sums = []
    for h in range(HEADS):
        total = part[row, h].astype(jnp.float32)
        for d in range(1, rows_n):
            total = total + part_in[lax.rem(row + d, rows_n), h].astype(jnp.float32)
        sums.append(total.astype(jnp.bfloat16))
    for z in range(cols_n):
        for p in range(packs):
            packed = jnp.zeros((padded, lanes), jnp.float32)
            for hh in range(pack):
                packed = packed + jnp.dot(
                    sums[p * pack + hh], pick(z, hh, (count, lanes), 1),
                    preferred_element_type=jnp.float32,
                )
            tile[z, p] = packed.astype(jnp.bfloat16)
    part_col = []
    for d in range(1, cols_n):
        peer = col_peer(d)
        part_col.append(remote(
            tile.at[peer[1]], tile_in.at[col], pc_send.at[d], pc_recv.at[d], peer
        ))
    for copy in part_col:
        copy.start()

    @pl.loop(chunks - held, chunks)
    def _(c):
        for copy in out_copies(c):
            copy.start()

    for copy in part_col:
        copy.wait_recv()
    total = tile[col].astype(jnp.float32)
    for d in range(1, cols_n):
        total = total + tile_in[lax.rem(col + d, cols_n)].astype(jnp.float32)
    for p in range(packs):
        for hh in range(pack):
            gb_ref[p * pack + hh] = total[p, 0:keys, hh * width:(hh + 1) * width]

    @pl.loop(0, chunks)
    def _(c):
        for copy in in_copies(c):
            copy.wait_send()
        for copy in out_copies(c):
            copy.wait()
        for copy in own_outs(c):
            copy.wait()

    for copy in bias_col + mask_col + bias_row + part_row + part_col:
        copy.wait_send()


def fused(rows_n, cols_n, query_proj, key_proj, value_proj, pair_bias, pair_mask, grad_out):
    rows, width, channels = query_proj.shape
    keys = pair_bias.shape[2]
    per, count = rows // cols_n, width * cols_n
    pack = 1
    while pack * 2 <= HEADS and pack * 2 * width <= 128:
        pack = pack * 2
    packs = HEADS // pack
    padded, lanes = round_up(keys, 16), round_up(pack * width, 128)
    mask_lanes = round_up(rows, 128)
    chunk = 2 if per % 2 == 0 else 1
    chunks = per // chunk
    bf16, f32 = jnp.bfloat16, jnp.float32
    anywhere = pl.BlockSpec(memory_space=pl.ANY)
    on_chip = pl.BlockSpec(memory_space=pltpu.VMEM)
    sem = pltpu.SemaphoreType.DMA
    tile_shape = pltpu.VMEM(query_proj.shape, bf16)
    gq, gk, gv, gb = pl.pallas_call(
        functools.partial(fused_kernel, rows_n, cols_n, pack),
        name="triangle_grads",
        out_shape=(
            tile_shape, tile_shape, tile_shape,
            jax.ShapeDtypeStruct((HEADS, keys, width), f32),
        ),
        in_specs=[anywhere] * 4 + [on_chip] * 2,
        out_specs=(on_chip,) * 4,
        scratch_shapes=[
            pltpu.VMEM((packs, padded, lanes), bf16),
            pltpu.VMEM((width, mask_lanes), bf16),
            pltpu.VMEM((4, per, count, channels), bf16),
            pltpu.VMEM((3, per, count, channels), bf16),
            pltpu.VMEM((rows_n, cols_n, packs, padded, lanes), bf16),
            pltpu.VMEM((count, mask_lanes), bf16),
            pltpu.VMEM((HEADS, count, count), f32),
            pltpu.VMEM((HEADS, count, count), f32),
            pltpu.VMEM((rows_n, HEADS, padded, count), bf16),
            pltpu.VMEM((rows_n, HEADS, padded, count), bf16),
            pltpu.VMEM((cols_n, packs, padded, lanes), bf16),
            pltpu.VMEM((cols_n, packs, padded, lanes), bf16),
            sem((chunks, cols_n, 4)), sem((chunks, cols_n, 4)),
            sem((chunks, cols_n, 3)), sem((chunks, cols_n, 3)),
            sem((cols_n,)), sem((cols_n,)),
            sem((rows_n,)), sem((rows_n,)),
            sem((cols_n,)), sem((cols_n,)),
            sem((rows_n,)), sem((rows_n,)),
            sem((cols_n,)), sem((cols_n,)),
            sem((6,)),
        ],
        compiler_params=pltpu.CompilerParams(collective_id=0, has_side_effects=True),
    )(query_proj, key_proj, value_proj, grad_out, jnp.transpose(pair_bias, (0, 2, 1)), pair_mask)
    return gq, gk, gv, jnp.transpose(gb, (0, 2, 1))


def choose(rows_n, cols_n):
    def run(*arrays):
        count = arrays[0].shape[1] * cols_n
        if count * count * 4 <= 512 * 1024 and arrays[0].shape[0] % cols_n == 0:
            return fused(rows_n, cols_n, *arrays)
        return local(*arrays)

    return run


def solution(mesh):
    placed = (
        P("row", "col", None),
        P("row", "col", None),
        P("row", "col", None),
        P(None, "col", "row"),
        P("row", "col"),
        P("row", "col", None),
    )
    return jax.shard_map(
        choose(mesh.shape["row"], mesh.shape["col"]),
        mesh=mesh,
        in_specs=placed,
        out_specs=(
            P("row", "col", None),
            P("row", "col", None),
            P("row", "col", None),
            P(None, "col", "row"),
        ),
        check_vma=False,
    )
```
